32 devices in a mesh: strip: 8 (over z, x), col: 4 (over y, core).
Axes of the slice: x: 2, y: 2, z: 4, core: 2. Of those that a mesh axis runs over, the one named last changes fastest.
Arguments:
- residuals: float32 [16, 64, 2560], P('strip'), may hold values from -6 to 6
- corr_rows: float32 [64], replicated, may hold values from 0.5 to 2
- corr_cols: float32 [2560], replicated, may hold values from 0.5 to 2
- row_anchor: int32 [16], replicated, may hold values from 0 to 64
- col_anchor: int32 [16], replicated, may hold values from 0 to 7680
- valid_first: int32 [16], replicated, may hold values from 0 to 15
- valid_end: int32 [16], replicated, may hold values from 49 to 64
- facet_of_slot: int32 [16], replicated, may hold values from 0 to 15, each once
Outputs:
- stitched: float32 [128, 10240], P('strip', 'col')
- column_power: float32 [10240], P('col')
The draws below stay inside these ranges and needn't reach their ends.
Inputs may be any that keep to these rules, and one draw needn't show every extreme that they name: facet_of_slot names each of the 16 facets exactly once.
All inputs are finite; a program needn't handle non-finite values.
Results may differ from the reference program's by a relative error of at most 0.0003.
Values sent between devices are 32-bit elements; how exact they have to be, the bound alone decides.
No kernel may reach another device: no remote copies, remote signals or barrier semaphores. Data moves between devices by JAX's collectives and lax.ppermute only.
A program may use at most 64 MiB of HBM per device.

```python
import math
import jax
import jax.numpy as jnp
from jax import lax

FW = 2560
FH = 64
FACETS = 16
MH = 128
MW = 10240


def with_ends(array, stream_key, low, largest):
    place = [jax.random.randint(jax.random.fold_in(stream_key, axis), (), 0, length) for axis, length in enumerate(array.shape)]
    longest = array.shape.index(max(array.shape))
    neighbour = place[:longest] + [(place[longest] + 1) % array.shape[longest]] + place[longest + 1:]
    return array.at[tuple(place)].set(low).at[tuple(neighbour)].set(largest)


def level_of(rng, shape, shards, smallest, high):
    loudness, own = 1.0, jax.random.fold_in(rng, 6)
    for dim, parts in shards:
        steps = jnp.exp(jax.random.uniform(jax.random.fold_in(own, dim), (parts,), jnp.float32, smallest / len(shards), high / len(shards)))
        loudness = loudness * jnp.repeat(steps, shape[dim] // parts).reshape([-1 if axis == dim else 1 for axis in range(len(shape))])
    return loudness


def scatter_about(rng, extent, deviation, most, split=(), dtype=jnp.bfloat16):
    entries = jax.random.normal(rng, extent, jnp.float32) * deviation
    if len(split) > 0:
        entries = level_of(rng, extent, split, -0.22, 0.18) * entries
    return jnp.clip(entries, min=-most, max=most).astype(dtype)


def setup_inputs(seed: int = 0) -> dict:
    keys = jax.random.split(jax.random.key(seed), 9)
    residuals = scatter_about(keys[0], (FACETS, FH, FW), 1.0, 6.0, ((0, 8),), jnp.float32)
    corr_rows = jnp.clip(jnp.exp(jax.random.uniform(keys[1], (FH,), jnp.float32, math.log(0.5), math.log(2.0))), 0.5, 2.0)
    corr_cols = jnp.clip(jnp.exp(jax.random.uniform(keys[2], (FW,), jnp.float32, math.log(0.5), math.log(2.0))), 0.5, 2.0)
    row_anchor = with_ends(jax.random.randint(keys[3], (FACETS,), 0, MH - FH + 1), jax.random.fold_in(keys[3], 1), 0, MH - FH).astype(jnp.int32)
    col_anchor = with_ends(jax.random.randint(keys[4], (FACETS,), 0, MW - FW + 1), jax.random.fold_in(keys[4], 1), 0, MW - FW).astype(jnp.int32)
    valid_first = with_ends(jax.random.randint(keys[5], (FACETS,), 0, FH // 4), jax.random.fold_in(keys[5], 1), 0, (FH // 4) - 1).astype(jnp.int32)
    valid_end = with_ends(jax.random.randint(keys[6], (FACETS,), 3 * FH // 4 + 1, FH + 1), jax.random.fold_in(keys[6], 1), 3 * FH // 4 + 1, FH).astype(jnp.int32)
    facet_of_slot = jax.random.permutation(keys[7], FACETS).astype(jnp.int32)
    return dict(residuals=residuals, corr_rows=corr_rows, corr_cols=corr_cols, row_anchor=row_anchor, col_anchor=col_anchor, valid_first=valid_first, valid_end=valid_end, facet_of_slot=facet_of_slot)


def tapers(count):
    position = (jnp.arange(count).astype(jnp.float32) + 0.5) / count
    return jnp.sin(jnp.pi * position) ** 2


def reference(residuals, corr_rows, corr_cols, row_anchor, col_anchor, valid_first, valid_end, facet_of_slot):
    facet_rows = residuals.shape[1]
    facet_cols = residuals.shape[2]
    row_index = jnp.arange(facet_rows).astype(jnp.int32)
    row_taper = tapers(facet_rows)
    col_taper = tapers(facet_cols)
    correction = corr_rows[:, None] * corr_cols[None, :]

    def accumulate(running, position):
        numerator, denominator = running
        facet_id = facet_of_slot[position]
        row_start = row_anchor[facet_id]
        col_start = col_anchor[facet_id]
        inside = (row_index >= valid_first[facet_id]) & (row_index < valid_end[facet_id])
        row_weight = jnp.where(inside, row_taper, 0.0)
        weight = row_weight[:, None] * col_taper[None, :]
        weighted = weight * correction * residuals[position]
        old_num = lax.dynamic_slice(numerator, (row_start, col_start), (facet_rows, facet_cols))
        numerator = lax.dynamic_update_slice(numerator, old_num + weighted, (row_start, col_start))
        old_den = lax.dynamic_slice(denominator, (row_start, col_start), (facet_rows, facet_cols))
        denominator = lax.dynamic_update_slice(denominator, old_den + weight, (row_start, col_start))
        return (numerator, denominator), None

    blank = jnp.zeros((MH, MW), jnp.float32)
    (numerator, denominator), _ = lax.scan(accumulate, (blank, blank), jnp.arange(FACETS).astype(jnp.int32))
    stitched = numerator / jnp.maximum(denominator, 0.5)
    column_power = jnp.mean(stitched * stitched, axis=0)
    return (stitched, column_power)
```

```python
import functools

import jax
import jax.numpy as jnp
import numpy as np
from jax import lax
from jax.experimental import pallas as pl
from jax.experimental.pallas import tpu as pltpu
from jax.sharding import PartitionSpec as P


def taper_row(count):
    position = (np.arange(count).astype(np.float32) + np.float32(0.5)) / np.float32(count)
    return (np.sin(np.float32(np.pi) * position) ** 2).astype(np.float32)[None, :]


def place_kernel(
    row_anchor, col_anchor, valid_first, valid_end, facet_of_slot,
    residuals, row_factor, row_taper, col_factor, col_taper, *bands, strip_count, group_count
):
    local_count, facet_rows, facet_cols = residuals.shape
    strip_rows = bands[0].shape[0]
    image_rows = strip_count * strip_rows
    strip_index = lax.axis_index("strip")
    group_index = lax.axis_index("col")
    image_row = lax.broadcasted_iota(jnp.int32, (image_rows, facet_rows), 0) ^ (
        strip_index * strip_rows
    )
    facet_row = lax.broadcasted_iota(jnp.int32, (image_rows, facet_rows), 1)
    column = lax.broadcasted_iota(jnp.int32, (1, facet_cols), 1)
    row_value = row_factor[...] * row_taper[...]
    col_value = col_factor[...] * col_taper[...]
    total = None
    for position in range(local_count):
        facet_id = facet_of_slot[strip_index * local_count + position]
        offset = col_anchor[facet_id] - group_index * facet_cols
        shift = lax.rem(offset + group_count * facet_cols, facet_cols)
        source = column - offset
        inside = (source >= 0) & (source < facet_cols)
        weighted = pltpu.roll(residuals[position] * col_value, shift, 1)
        weighted = jnp.where(inside, weighted, 0.0)
        hit = (
            (image_row - row_anchor[facet_id] == facet_row)
            & (facet_row >= valid_first[facet_id])
            & (facet_row < valid_end[facet_id])
        )
        place = jnp.where(hit, row_value, 0.0)
        part = jnp.dot(
            place, weighted,
            precision=lax.Precision.HIGHEST, preferred_element_type=jnp.float32,
        )
        total = part if total is None else total + part
    for k, band in enumerate(bands):
        band[...] = total[k * strip_rows:(k + 1) * strip_rows]


def body(
    residuals, corr_rows, corr_cols, row_anchor, col_anchor, valid_first, valid_end, facet_of_slot
):
    local_count, facet_rows, facet_cols = residuals.shape
    strip_count = lax.axis_size("strip")
    group_count = lax.axis_size("col")
    strip_rows = facet_rows // 4
    image_rows = strip_count * strip_rows
    strip_index = lax.axis_index("strip")
    group_index = lax.axis_index("col")
    assert strip_count & (strip_count - 1) == 0 and strip_rows & (strip_rows - 1) == 0
    smem = pl.BlockSpec(memory_space=pltpu.SMEM)
    vmem = pl.BlockSpec(memory_space=pltpu.VMEM)
    bands = pl.pallas_call(
        functools.partial(place_kernel, strip_count=strip_count, group_count=group_count),
        out_shape=[jax.ShapeDtypeStruct((strip_rows, facet_cols), jnp.float32)] * strip_count,
        in_specs=[smem] * 5 + [vmem] * 5,
        out_specs=[vmem] * strip_count,
        name="place",
    )(
        row_anchor, col_anchor, valid_first, valid_end, facet_of_slot,
        residuals, corr_rows[None, :], taper_row(facet_rows), corr_cols[None, :],
        taper_row(facet_cols),
    )

    def flip(value, k):
        return lax.ppermute(value, "strip", [(i, i ^ k) for i in range(strip_count)])

    got = [flip(bands[k], k) for k in range(strip_count - 1, 0, -1)]

    row_local = strip_index * strip_rows + jnp.arange(strip_rows)
    row_pos = row_local[None, :] - row_anchor[:, None]
    row_inside = (row_pos >= valid_first[:, None]) & (row_pos < valid_end[:, None])
    row_value = jnp.sin(jnp.pi * (row_pos.astype(jnp.float32) + 0.5) / facet_rows) ** 2
    row_part = jnp.where(row_inside, row_value, 0.0)
    col_local = group_index * facet_cols + jnp.arange(facet_cols)
    col_pos = col_local[None, :] - col_anchor[:, None]
    col_inside = (col_pos >= 0) & (col_pos < facet_cols)
    col_value = jnp.sin(jnp.pi * (col_pos.astype(jnp.float32) + 0.5) / facet_cols) ** 2
    col_part = jnp.where(col_inside, col_value, 0.0)
    denominator = jnp.einsum("fv,fu->vu", row_part, col_part, precision=lax.Precision.HIGHEST)

    numerator = bands[0]
    for value in got:
        numerator = numerator + value
    stitched = numerator / jnp.maximum(denominator, 0.5)
    power = jnp.sum(stitched * stitched, axis=0)
    k = 1
    while k < strip_count:
        power = power + flip(power, k)
        k *= 2
    return (stitched, power / image_rows)


def solution(mesh):
    in_specs = (P("strip", None, None), P(), P(), P(), P(), P(), P(), P())
    out_specs = (P("strip", "col"), P("col"))
    return jax.shard_map(body, mesh=mesh, in_specs=in_specs, out_specs=out_specs, check_vma=False)
```

```python
import functools

import jax
import jax.numpy as jnp
import numpy as np
from jax import lax
from jax.experimental import pallas as pl
from jax.experimental.pallas import tpu as pltpu
from jax.sharding import PartitionSpec as P


def taper_row(count):
    position = (np.arange(count).astype(np.float32) + np.float32(0.5)) / np.float32(count)
    return (np.sin(np.float32(np.pi) * position) ** 2).astype(np.float32)[None, :]


def place_kernel(
    row_anchor, col_anchor, valid_first, valid_end, facet_of_slot,
    residuals, row_factor, row_taper, col_factor, col_taper, *bands, strip_count, group_count
):
    local_count, facet_rows, facet_cols = residuals.shape
    strip_rows = bands[0].shape[0]
    image_rows = strip_count * strip_rows
    strip_index = lax.axis_index("strip")
    group_index = lax.axis_index("col")
    image_row = lax.broadcasted_iota(jnp.int32, (image_rows, facet_rows), 0) ^ (
        strip_index * strip_rows
    )
    facet_row = lax.broadcasted_iota(jnp.int32, (image_rows, facet_rows), 1)
    column = lax.broadcasted_iota(jnp.int32, (1, facet_cols), 1)
    row_value = row_factor[...] * row_taper[...]
    col_value = col_factor[...] * col_taper[...]
    total = None
    for position in range(local_count):
        facet_id = facet_of_slot[strip_index * local_count + position]
        offset = col_anchor[facet_id] - group_index * facet_cols
        shift = lax.rem(offset + group_count * facet_cols, facet_cols)
        source = column - offset
        inside = (source >= 0) & (source < facet_cols)
        weighted = pltpu.roll(residuals[position] * col_value, shift, 1)
        weighted = jnp.where(inside, weighted, 0.0)
        hit = (
            (image_row - row_anchor[facet_id] == facet_row)
            & (facet_row >= valid_first[facet_id])
            & (facet_row < valid_end[facet_id])
        )
        place = jnp.where(hit, row_value, 0.0)
        part = jnp.dot(
            place, weighted,
            precision=lax.Precision.HIGHEST, preferred_element_type=jnp.float32,
        )
        total = part if total is None else total + part
    for k, band in enumerate(bands):
        band[...] = total[k * strip_rows:(k + 1) * strip_rows]


def body(
    residuals, corr_rows, corr_cols, row_anchor, col_anchor, valid_first, valid_end, facet_of_slot
):
    local_count, facet_rows, facet_cols = residuals.shape
    strip_count = lax.axis_size("strip")
    group_count = lax.axis_size("col")
    strip_rows = facet_rows // 4
    image_rows = strip_count * strip_rows
    strip_index = lax.axis_index("strip")
    group_index = lax.axis_index("col")
    assert strip_count & (strip_count - 1) == 0 and strip_rows & (strip_rows - 1) == 0
    smem = pl.BlockSpec(memory_space=pltpu.SMEM)
    vmem = pl.BlockSpec(memory_space=pltpu.VMEM)
    bands = pl.pallas_call(
        functools.partial(place_kernel, strip_count=strip_count, group_count=group_count),
        out_shape=[jax.ShapeDtypeStruct((strip_rows, facet_cols), jnp.float32)] * strip_count,
        in_specs=[smem] * 5 + [vmem] * 5,
        out_specs=[vmem] * strip_count,
        name="place",
    )(
        row_anchor, col_anchor, valid_first, valid_end, facet_of_slot,
        residuals, corr_rows[None, :], taper_row(facet_rows), corr_cols[None, :],
        taper_row(facet_cols),
    )

    def flip(value, k):
        return lax.ppermute(value, "strip", [(i, i ^ k) for i in range(strip_count)])

    half = strip_count // 2
    far = [flip(bands[m ^ half], m) for m in range(half - 1, 0, -1)]
    near = [flip(bands[m], m) for m in range(half - 1, 0, -1)]
    crossing = bands[half]
    for value in far:
        crossing = crossing + value
    got = near + [flip(crossing, half)]

    row_local = strip_index * strip_rows + jnp.arange(strip_rows)
    row_pos = row_local[None, :] - row_anchor[:, None]
    row_inside = (row_pos >= valid_first[:, None]) & (row_pos < valid_end[:, None])
    row_value = jnp.sin(jnp.pi * (row_pos.astype(jnp.float32) + 0.5) / facet_rows) ** 2
    row_part = jnp.where(row_inside, row_value, 0.0)
    col_local = group_index * facet_cols + jnp.arange(facet_cols)
    col_pos = col_local[None, :] - col_anchor[:, None]
    col_inside = (col_pos >= 0) & (col_pos < facet_cols)
    col_value = jnp.sin(jnp.pi * (col_pos.astype(jnp.float32) + 0.5) / facet_cols) ** 2
    col_part = jnp.where(col_inside, col_value, 0.0)
    denominator = jnp.einsum("fv,fu->vu", row_part, col_part, precision=lax.Precision.HIGHEST)

    denominator = lax.optimization_barrier(jnp.maximum(denominator, 0.5))
    numerator = bands[0]
    for value in got:
        numerator = numerator + value
    stitched = numerator / denominator
    power = jnp.sum(stitched * stitched, axis=0)
    k = 1
    while k < strip_count:
        if 4 * k <= strip_count:
            parts = [flip(power, k * m) for m in (3, 2, 1)]
            power = power + parts[0] + parts[1] + parts[2]
            k *= 4
        else:
            power = power + flip(power, k)
            k *= 2
    return (stitched, power / image_rows)


def solution(mesh):
    in_specs = (P("strip", None, None), P(), P(), P(), P(), P(), P(), P())
    out_specs = (P("strip", "col"), P("col"))
    return jax.shard_map(body, mesh=mesh, in_specs=in_specs, out_specs=out_specs, check_vma=False)
```

```python
import functools

import jax
import jax.numpy as jnp
import numpy as np
from jax import lax
from jax.experimental import pallas as pl
from jax.experimental.pallas import tpu as pltpu
from jax.sharding import PartitionSpec as P


def taper_row(count):
    position = (np.arange(count).astype(np.float32) + np.float32(0.5)) / np.float32(count)
    return (np.sin(np.float32(np.pi) * position) ** 2).astype(np.float32)[None, :]


def place_kernel(
    row_anchor, col_anchor, valid_first, valid_end, facet_of_slot,
    residuals, row_factor, row_taper, col_factor, col_taper, *bands, strip_count, group_count
):
    local_count, facet_rows, facet_cols = residuals.shape
    strip_rows = bands[0].shape[0]
    image_rows = strip_count * strip_rows
    strip_index = lax.axis_index("strip")
    group_index = lax.axis_index("col")
    image_row = lax.broadcasted_iota(jnp.int32, (image_rows, facet_rows), 0) ^ (
        strip_index * strip_rows
    )
    facet_row = lax.broadcasted_iota(jnp.int32, (image_rows, facet_rows), 1)
    column = lax.broadcasted_iota(jnp.int32, (1, facet_cols), 1)
    square = (facet_rows, facet_rows)
    row_number = lax.broadcasted_iota(jnp.int32, square, 0)
    diagonal = row_number == lax.broadcasted_iota(jnp.int32, square, 1)
    row_spread = jnp.where(diagonal, row_factor[...] * row_taper[...], 0.0)
    row_value = jnp.sum(row_spread, axis=1, keepdims=True)
    row_number = row_number[:, :1]
    col_value = col_factor[...].reshape(1, facet_cols) * col_taper[...]
    places = []
    pieces = []
    for position in range(local_count):
        facet_id = facet_of_slot[strip_index * local_count + position]
        offset = col_anchor[facet_id] - group_index * facet_cols
        shift = lax.rem(offset + group_count * facet_cols, facet_cols)
        source = column - offset
        inside = (source >= 0) & (source < facet_cols)
        valid = (row_number >= valid_first[facet_id]) & (row_number < valid_end[facet_id])
        col_shifted = jnp.where(inside, pltpu.roll(col_value, shift, 1), 0.0)
        weighted = pltpu.roll(residuals[position], shift, 1) * col_shifted
        weighted = weighted * jnp.where(valid, row_value, 0.0)
        high = weighted.astype(jnp.bfloat16)
        low = (weighted - high.astype(jnp.float32)).astype(jnp.bfloat16)
        hit = image_row - row_anchor[facet_id] == facet_row
        place = jnp.where(hit, 1.0, 0.0).astype(jnp.bfloat16)
        places += [place, place]
        pieces += [high, low]
    total = jnp.dot(
        jnp.concatenate(places, axis=1), jnp.concatenate(pieces, axis=0),
        preferred_element_type=jnp.float32,
    )
    for k, band in enumerate(bands):
        band[...] = total[k * strip_rows:(k + 1) * strip_rows]


def body(
    residuals, corr_rows, corr_cols, row_anchor, col_anchor, valid_first, valid_end, facet_of_slot
):
    local_count, facet_rows, facet_cols = residuals.shape
    strip_count = lax.axis_size("strip")
    group_count = lax.axis_size("col")
    strip_rows = facet_rows // 4
    image_rows = strip_count * strip_rows
    strip_index = lax.axis_index("strip")
    group_index = lax.axis_index("col")
    assert strip_count & (strip_count - 1) == 0 and strip_rows & (strip_rows - 1) == 0
    smem = pl.BlockSpec(memory_space=pltpu.SMEM)
    vmem = pl.BlockSpec(memory_space=pltpu.VMEM)
    on_chip = image_rows * facet_cols * 4 <= 2 ** 21
    make = pltpu.VMEM if on_chip else jax.ShapeDtypeStruct
    bands = pl.pallas_call(
        functools.partial(place_kernel, strip_count=strip_count, group_count=group_count),
        out_shape=[make((strip_rows, facet_cols), jnp.float32)] * strip_count,
        in_specs=[smem] * 5 + [vmem] * 5,
        out_specs=[vmem] * strip_count,
        name="place",
    )(
        row_anchor, col_anchor, valid_first, valid_end, facet_of_slot,
        residuals, corr_rows[None, :], taper_row(facet_rows), corr_cols,
        taper_row(facet_cols),
    )

    def flip(value, k):
        return lax.ppermute(value, "strip", [(i, i ^ k) for i in range(strip_count)])

    half = strip_count // 2
    far = [flip(bands[m ^ half], m) for m in range(half - 1, 0, -1)]
    near = [flip(bands[m], m) for m in range(half - 1, 0, -1)]
    crossing = bands[half]
    for value in far:
        crossing = crossing + value
    got = near + [flip(crossing, half)]

    row_local = strip_index * strip_rows + jnp.arange(strip_rows)
    row_pos = row_local[None, :] - row_anchor[:, None]
    row_inside = (row_pos >= valid_first[:, None]) & (row_pos < valid_end[:, None])
    row_value = jnp.sin(jnp.pi * (row_pos.astype(jnp.float32) + 0.5) / facet_rows) ** 2
    row_part = jnp.where(row_inside, row_value, 0.0)
    col_local = group_index * facet_cols + jnp.arange(facet_cols)
    col_pos = col_local[None, :] - col_anchor[:, None]
    col_inside = (col_pos >= 0) & (col_pos < facet_cols)
    col_value = jnp.sin(jnp.pi * (col_pos.astype(jnp.float32) + 0.5) / facet_cols) ** 2
    col_part = jnp.where(col_inside, col_value, 0.0)
    denominator = jnp.einsum("fv,fu->vu", row_part, col_part, precision=lax.Precision.HIGHEST)

    denominator = lax.optimization_barrier(jnp.maximum(denominator, 0.5))
    numerator = bands[0]
    for value in got:
        numerator = numerator + value
    stitched = numerator / denominator
    power = jnp.sum(stitched * stitched, axis=0)
    k = 1
    while k < strip_count:
        if 4 * k <= strip_count:
            parts = [flip(power, k * m) for m in (3, 2, 1)]
            power = power + parts[0] + parts[1] + parts[2]
            k *= 4
        else:
            power = power + flip(power, k)
            k *= 2
    return (stitched, power / image_rows)


def solution(mesh):
    in_specs = (P("strip", None, None), P(), P(), P(), P(), P(), P(), P())
    out_specs = (P("strip", "col"), P("col"))
    return jax.shard_map(body, mesh=mesh, in_specs=in_specs, out_specs=out_specs, check_vma=False)
```

```python
import functools

import jax
import jax.numpy as jnp
import numpy as np
from jax import lax
from jax.experimental import pallas as pl
from jax.experimental.pallas import tpu as pltpu
from jax.sharding import PartitionSpec as P


def taper_row(count):
    position = (np.arange(count).astype(np.float32) + np.float32(0.5)) / np.float32(count)
    return (np.sin(np.float32(np.pi) * position) ** 2).astype(np.float32)[None, :]


def place_kernel(
    row_anchor, col_anchor, valid_first, valid_end, facet_of_slot,
    residuals, row_factor, row_taper, col_factor, col_taper, *bands, strip_count, group_count
):
    local_count, facet_rows, facet_cols = residuals.shape
    strip_rows = bands[0].shape[0]
    image_rows = strip_count * strip_rows
    strip_index = lax.axis_index("strip")
    group_index = lax.axis_index("col")
    image_row = lax.broadcasted_iota(jnp.int32, (image_rows, facet_rows), 0) ^ (
        strip_index * strip_rows
    )
    facet_row = lax.broadcasted_iota(jnp.int32, (image_rows, facet_rows), 1)
    column = lax.broadcasted_iota(jnp.int32, (1, facet_cols), 1)
    square = (facet_rows, facet_rows)
    row_number = lax.broadcasted_iota(jnp.int32, square, 0)
    diagonal = row_number == lax.broadcasted_iota(jnp.int32, square, 1)
    row_spread = jnp.where(diagonal, row_factor[...] * row_taper[...], 0.0)
    row_value = jnp.sum(row_spread, axis=1, keepdims=True)
    row_number = row_number[:, :1]
    col_value = col_factor[...].reshape(1, facet_cols) * col_taper[...]
    places = []
    pieces = []
    for position in range(local_count):
        facet_id = facet_of_slot[strip_index * local_count + position]
        offset = col_anchor[facet_id] - group_index * facet_cols
        shift = lax.rem(offset + group_count * facet_cols, facet_cols)
        source = column - offset
        inside = (source >= 0) & (source < facet_cols)
        valid = (row_number >= valid_first[facet_id]) & (row_number < valid_end[facet_id])
        col_shifted = jnp.where(inside, pltpu.roll(col_value, shift, 1), 0.0)
        weighted = pltpu.roll(residuals[position], shift, 1) * col_shifted
        weighted = weighted * jnp.where(valid, row_value, 0.0)
        high = weighted.astype(jnp.bfloat16)
        low = (weighted - high.astype(jnp.float32)).astype(jnp.bfloat16)
        hit = image_row - row_anchor[facet_id] == facet_row
        place = jnp.where(hit, 1.0, 0.0).astype(jnp.bfloat16)
        places += [place, place]
        pieces += [high, low]
    total = jnp.dot(
        jnp.concatenate(places, axis=1), jnp.concatenate(pieces, axis=0),
        preferred_element_type=jnp.float32,
    )
    for k, band in enumerate(bands):
        band[...] = total[k * strip_rows:(k + 1) * strip_rows]


def body(
    residuals, corr_rows, corr_cols, row_anchor, col_anchor, valid_first, valid_end, facet_of_slot
):
    local_count, facet_rows, facet_cols = residuals.shape
    strip_count = lax.axis_size("strip")
    group_count = lax.axis_size("col")
    strip_rows = facet_rows // 4
    image_rows = strip_count * strip_rows
    strip_index = lax.axis_index("strip")
    group_index = lax.axis_index("col")
    assert strip_count & (strip_count - 1) == 0 and strip_rows & (strip_rows - 1) == 0
    smem = pl.BlockSpec(memory_space=pltpu.SMEM)
    vmem = pl.BlockSpec(memory_space=pltpu.VMEM)
    on_chip = image_rows * facet_cols * 4 <= 2 ** 21
    make = pltpu.VMEM if on_chip else jax.ShapeDtypeStruct
    bands = pl.pallas_call(
        functools.partial(place_kernel, strip_count=strip_count, group_count=group_count),
        out_shape=[make((strip_rows, facet_cols), jnp.float32)] * strip_count,
        in_specs=[smem] * 5 + [vmem] * 5,
        out_specs=[vmem] * strip_count,
        name="place",
    )(
        row_anchor, col_anchor, valid_first, valid_end, facet_of_slot,
        residuals, corr_rows[None, :], taper_row(facet_rows), corr_cols,
        taper_row(facet_cols),
    )

    def flip(value, k):
        return lax.ppermute(value, "strip", [(i, i ^ k) for i in range(strip_count)])

    half = strip_count // 2
    far = [flip(bands[m ^ half], m) for m in range(1, half)]
    near = [flip(bands[m], m) for m in range(half - 1, 0, -1)]
    crossing = bands[half]
    for value in far:
        crossing = crossing + value
    got = near + [flip(crossing, half)]

    row_local = strip_index * strip_rows + jnp.arange(strip_rows)
    row_pos = row_local[None, :] - row_anchor[:, None]
    row_inside = (row_pos >= valid_first[:, None]) & (row_pos < valid_end[:, None])
    row_value = jnp.sin(jnp.pi * (row_pos.astype(jnp.float32) + 0.5) / facet_rows) ** 2
    row_part = jnp.where(row_inside, row_value, 0.0)
    col_local = group_index * facet_cols + jnp.arange(facet_cols)
    col_pos = col_local[None, :] - col_anchor[:, None]
    col_inside = (col_pos >= 0) & (col_pos < facet_cols)
    col_value = jnp.sin(jnp.pi * (col_pos.astype(jnp.float32) + 0.5) / facet_cols) ** 2
    col_part = jnp.where(col_inside, col_value, 0.0)
    denominator = jnp.einsum("fv,fu->vu", row_part, col_part, precision=lax.Precision.HIGHEST)

    denominator = lax.optimization_barrier(jnp.maximum(denominator, 0.5))
    numerator = bands[0]
    for value in got:
        numerator = numerator + value
    stitched = numerator / denominator
    power = jnp.sum(stitched * stitched, axis=0)
    k = 1
    while k < strip_count:
        if 4 * k <= strip_count:
            parts = [flip(power, k * m) for m in (3, 2, 1)]
            power = power + parts[0] + parts[1] + parts[2]
            k *= 4
        else:
            power = power + flip(power, k)
            k *= 2
    return (stitched, power / image_rows)


def solution(mesh):
    in_specs = (P("strip", None, None), P(), P(), P(), P(), P(), P(), P())
    out_specs = (P("strip", "col"), P("col"))
    return jax.shard_map(body, mesh=mesh, in_specs=in_specs, out_specs=out_specs, check_vma=False)
```
